32 devices in a mesh: section: 8 (over z, x), tensor: 4 (over y, core).
Axes of the slice: x: 2, y: 2, z: 4, core: 2. Of those that a mesh axis runs over, the one named last changes fastest.
Arguments:
- hidden: bfloat16 [32, 8192], P(('section', 'tensor')), may hold values from -12 to 12
- weight: bfloat16 [16384, 8192], P(('section', 'tensor')), may hold values from -1 to 1
- targets: int32 [32], replicated, may hold values from 0 to 16383
- loss_grad: float32 [32], P(('section', 'tensor')), may hold values from 8 to 64
Outputs:
- token_loss: float32 [32], P(('section', 'tensor'))
- hidden_grad: bfloat16 [32, 8192], P(('section', 'tensor'))
The draws below stay inside these ranges and needn't reach their ends.
All inputs are finite; a program needn't handle non-finite values.
Results may differ from the reference program's by a relative error of at most 0.0039.
Values may be sent and summed in bfloat16 or wider, within the bound.
No kernel may reach another device: no remote copies, remote signals or barrier semaphores. Data moves between devices by JAX's collectives and lax.ppermute only.
A program may use at most 64 MiB of HBM per device.

```python
import math
import jax
import jax.numpy as jnp
from jax import lax

D = 8192
TOKENS = 32
VOCAB = 16384


def weight_matrix(key):
    base_key = jax.random.fold_in(key, 11)
    keys = jax.random.split(base_key, 1)
    ramp = 1.0 + 0.25 * jnp.arange(VOCAB, dtype=jnp.float32) / VOCAB
    entries = jax.random.truncated_normal(keys[0], -6.0, 6.0, (VOCAB, D), jnp.float32)
    return (entries * ramp[:, None] * (3.0 / math.sqrt(D))).astype(jnp.bfloat16)


def draw_weight(key, part):
    return weight_matrix(key)


def draw_hidden(key, part):
    keys = jax.random.split(jax.random.fold_in(key, 23), 1)
    limit = 12.0 * max(1, 512 // D)
    values = jax.random.truncated_normal(keys[0], -6.0, 6.0, (TOKENS, D), jnp.float32)
    values = jnp.clip(values, -limit, limit)
    return values.astype(jnp.bfloat16)


def place_ends(array, stream_key, least, high):
    longest = array.shape.index(max(array.shape))
    spots = []
    for shift in (0, 1):
        where = [jax.random.randint(jax.random.fold_in(stream_key, axis), (), 0, length) for axis, length in enumerate(array.shape)]
        where[longest] = (where[longest] + shift) % array.shape[longest]
        spots.append(tuple(where))
    return array.at[spots[0]].set(least).at[spots[1]].set(high)


def steps_of(stream_key, dims, cuts, smallest, high):
    def one(dim, blocks):
        steps = jax.random.uniform(jax.random.fold_in(jax.random.fold_in(stream_key, 6), dim), (blocks,), jnp.float32, smallest / len(cuts), high / len(cuts))
        return jnp.repeat(jnp.exp(steps), dims[dim] // blocks).reshape((-1,) + (1,) * (len(dims) - dim - 1))

    level = one(*cuts[0])
    for cut in cuts[1:]:
        level = level * one(*cut)
    return level


def setup_inputs(seed: int = 0) -> dict:
    arg_keys = jax.random.split(jax.random.key(seed), 5)
    return {
        "hidden": draw_hidden(jax.random.fold_in(arg_keys[4], 71), 0),
        "weight": draw_weight(jax.random.fold_in(arg_keys[4], 71), 0),
        "targets": place_ends(jax.random.randint(arg_keys[2], (TOKENS,), 0, VOCAB), jax.random.fold_in(arg_keys[2], 1), 0, VOCAB - 1).astype(jnp.int32),
        "loss_grad": jnp.clip(jnp.exp(math.log(64.0) - 2.0794415 * jax.random.uniform(arg_keys[3], (TOKENS,), jnp.float32) ** steps_of(arg_keys[3], (TOKENS,), ((0, 32),), -0.2, 0.2)), 8.0, 64.0),
    }


def reference(hidden, weight, targets, loss_grad):
    logits = lax.dot_general(hidden, weight, (((1,), (1,)), ((), ())), preferred_element_type=jnp.float32)
    row_max = jnp.max(logits, axis=1)
    shifted = jnp.exp(logits - row_max[:, None])
    exp_total = jnp.sum(shifted, axis=1)
    target_logit = jnp.take_along_axis(logits, targets[:, None].astype(jnp.int32), axis=1)[:, 0]
    token_loss = row_max + jnp.log(exp_total) - target_logit
    columns = lax.broadcasted_iota(jnp.int32, logits.shape, 1)
    one_hot = (columns == targets[:, None].astype(jnp.int32)).astype(jnp.float32)
    probs_grad = (shifted / exp_total[:, None] - one_hot).astype(jnp.bfloat16)
    grad_sum = jnp.dot(probs_grad, weight, preferred_element_type=jnp.float32)
    hidden_grad = (loss_grad[:, None] * grad_sum).astype(jnp.bfloat16)
    return (token_loss, hidden_grad)
```

```python
import functools
import math

import jax
import jax.numpy as jnp
from jax import lax
from jax.experimental import pallas as pl
from jax.experimental.pallas import tpu as pltpu
from jax.sharding import PartitionSpec as P

AXES = ("section", "tensor")
LANES = 128
F32 = jnp.float32
BF16 = jnp.bfloat16
VMEM = pl.BlockSpec(memory_space=pltpu.VMEM)
PARAMS = pltpu.CompilerParams(vmem_limit_bytes=32 * 2**20)


def bit_groups(devices):
    bits = devices.bit_length() - 1
    groups, top = [], bits
    while top > 1:
        low = max(1, top - 2)
        groups.append((low, top - low))
        top = low
    return groups + [(0, 1)]


def swap(array, mask, devices):
    return lax.ppermute(array, AXES, [(i, i ^ mask) for i in range(devices)])


def split3(value):
    parts = []
    for _ in range(3):
        part = value.astype(BF16).astype(F32)
        parts.append(part)
        value = value - part
    return parts


def pack(values, rows):
    lane = lax.broadcasted_iota(jnp.int32, (rows, LANES), 1)
    block = jnp.zeros((rows, LANES), F32)
    for i, part in enumerate(p for v in values for p in split3(v)):
        block = jnp.where(lane == i, part, block)
    return block.astype(BF16)


def unpack(block):
    block = block.astype(F32)
    return [
        block[:, 3 * i : 3 * i + 1] + block[:, 3 * i + 1 : 3 * i + 2] + block[:, 3 * i + 2 : 3 * i + 3]
        for i in range(3)
    ]


def owner_of(row, order):
    mask, place = jnp.zeros_like(row), 0
    for low, count in order:
        mask = mask | (((row >> place) & ((1 << count) - 1)) << low)
        place += count
    return mask


def local_kernel(order, tok_dev, *refs):
    *hidden_refs, weight_ref, targets_ref, keep_ref, give_ref, acc = refs
    hidden = jnp.concatenate([ref[...] for ref in hidden_refs], 0)
    rows, depth = hidden.shape
    vocab = weight_ref.shape[0]
    me = lax.axis_index(AXES)
    logits = lax.dot_general(
        hidden, weight_ref[...], (((1,), (1,)), ((), ())), preferred_element_type=F32
    )
    tokens = targets_ref.shape[1]
    row = lax.broadcasted_iota(jnp.int32, (rows, tokens), 0)
    token = (me ^ owner_of(row // tok_dev, order)) * tok_dev + row % tok_dev
    column = lax.broadcasted_iota(jnp.int32, (rows, tokens), 1)
    target = jnp.sum(
        jnp.where(column == token, targets_ref[...], 0), axis=1, keepdims=True
    ) - me * vocab
    hit = lax.broadcasted_iota(jnp.int32, (rows, vocab), 1) == target
    largest = jnp.max(logits, axis=1, keepdims=True)
    shifted = jnp.exp(logits - largest)
    total = jnp.sum(shifted, axis=1, keepdims=True)
    at_target = jnp.sum(jnp.where(hit, logits, 0.0), axis=1, keepdims=True)
    both = jnp.concatenate([shifted.astype(BF16), hit.astype(F32).astype(BF16)], 0)
    half = rows // 2
    stats = pack((largest, total, at_target), rows)
    keep_ref[:, 2 * depth :] = stats[:half]
    give_ref[:, 2 * depth :] = stats[half:]
    step = min(depth, 1024)
    for at in range(0, depth, step):
        out = jnp.dot(both, weight_ref[:, at : at + step], preferred_element_type=F32).astype(BF16)
        keep_ref[:, at : at + step] = out[:half]
        give_ref[:, at : at + step] = out[half:rows]
        keep_ref[:, depth + at : depth + at + step] = out[rows : rows + half]
        give_ref[:, depth + at : depth + at + step] = out[rows + half :]


def merged(refs):
    stats = [unpack(ref[:, -LANES:]) for ref in refs]
    largest = functools.reduce(jnp.maximum, [s[0] for s in stats])
    scales = [jnp.exp(s[0] - largest) for s in stats]
    total = sum(a * s[1] for a, s in zip(scales, stats))
    at_target = sum(s[2] for s in stats)
    return scales, largest, total, at_target


def merge_kernel(parts, *refs):
    ins, outs = refs[:parts], refs[parts:]
    scales, *stats = merged(ins)
    rows, width = ins[0].shape
    depth = (width - LANES) // 2
    each = rows // len(outs)

    def put(at, size, value):
        for i, out in enumerate(outs):
            out[:, at : at + size] = value[i * each : (i + 1) * each]

    put(2 * depth, LANES, pack(stats, rows))
    put(0, depth, sum(a * ref[:, :depth].astype(F32) for a, ref in zip(scales, ins)).astype(BF16))
    put(depth, depth, sum(ref[:, depth : 2 * depth].astype(F32) for ref in ins).astype(BF16))


def last_kernel(parts, *refs):
    ins, (scale_ref, loss_ref, grad_ref) = refs[:parts], refs[parts:]
    scales, largest, total, at_target = merged(ins)
    width = ins[0].shape[1]
    depth = (width - LANES) // 2
    loss_ref[...] = jnp.broadcast_to(largest + jnp.log(total) - at_target, loss_ref.shape)
    summed = sum(a * ref[:, :depth].astype(F32) for a, ref in zip(scales, ins))
    hot = sum(ref[:, depth : 2 * depth].astype(F32) for ref in ins)
    grad_ref[...] = (scale_ref[...] * (summed / total - hot)).astype(BF16)


def call(kernel, ins, outs, scratch=()):
    return pl.pallas_call(
        kernel,
        out_shape=outs,
        in_specs=[VMEM] * len(ins),
        out_specs=jax.tree.map(lambda _: VMEM, outs),
        scratch_shapes=list(scratch),
        compiler_params=PARAMS,
    )(*ins)


def shards(devices, hidden, weight, targets, loss_grad):
    tok_dev, depth = hidden.shape
    groups = bit_groups(devices)
    pieces = [hidden]
    for low, count in groups:
        whole = jnp.concatenate(pieces, 0) if len(pieces) > 1 else pieces[0]
        pieces = [whole] + [swap(whole, k << low, devices) for k in range(1, 1 << count)]
    rows = devices * tok_dev
    width = 2 * depth + LANES
    half = jax.ShapeDtypeStruct((rows // 2, width), BF16)
    keep, give = call(
        functools.partial(local_kernel, groups, tok_dev),
        [*pieces, weight, targets[None, :]],
        (half, half),
        [pltpu.VMEM((8, LANES), F32)],
    )
    parts = [keep, swap(give, 1, devices)]
    for low, count in reversed(groups[:-1]):
        peers = 1 << count
        size = parts[0].shape[0] // peers
        outs = call(
            functools.partial(merge_kernel, len(parts)),
            parts,
            tuple(jax.ShapeDtypeStruct((size, width), BF16) for _ in range(peers)),
        )
        parts = [outs[0]] + [swap(outs[k], k << low, devices) for k in range(1, peers)]
    loss, grad = call(
        functools.partial(last_kernel, len(parts)),
        [*parts, loss_grad[:, None]],
        (
            jax.ShapeDtypeStruct((tok_dev, LANES), F32),
            jax.ShapeDtypeStruct((tok_dev, depth), BF16),
        ),
    )
    return loss[:, 0], grad


def solution(mesh):
    devices = math.prod(mesh.shape[axis] for axis in AXES)
    return jax.shard_map(
        functools.partial(shards, devices),
        mesh=mesh,
        in_specs=(P(AXES, None), P(AXES, None), P(), P(AXES)),
        out_specs=(P(AXES), P(AXES, None)),
        check_vma=False,
    )
```

```python
import functools
import math

import jax
import jax.numpy as jnp
from jax import lax
from jax.experimental import pallas as pl
from jax.experimental.pallas import tpu as pltpu
from jax.sharding import PartitionSpec as P


AXES = ("section", "tensor")
LANES = 128
F32 = jnp.float32
BF16 = jnp.bfloat16
VMEM = pl.BlockSpec(memory_space=pltpu.VMEM)
HBM = pl.BlockSpec(memory_space=pl.ANY)
SMEM = pl.BlockSpec(memory_space=pltpu.SMEM)
PARAMS = pltpu.CompilerParams(vmem_limit_bytes=32 * 2**20)
LOAD_PARAMS = pltpu.CompilerParams(vmem_limit_bytes=44 * 2**20)


def bit_groups(devices):
    bits = devices.bit_length() - 1
    groups, top = [], bits
    while top > 1:
        low = max(1, top - 2)
        groups.append((low, top - low))
        top = low
    return groups + [(0, 1)]


def swap(array, mask, devices):
    return lax.ppermute(array, AXES, [(i, i ^ mask) for i in range(devices)])


def split3(value):
    parts = []
    for _ in range(3):
        part = value.astype(BF16).astype(F32)
        parts.append(part)
        value = value - part
    return parts


def pack(values, rows):
    lane = lax.broadcasted_iota(jnp.int32, (rows, LANES), 1)
    block = jnp.zeros((rows, LANES), F32)
    for i, part in enumerate(p for v in values for p in split3(v)):
        block = jnp.where(lane == i, part, block)
    return block.astype(BF16)


def unpack(block):
    block = block.astype(F32)
    return [
        block[:, 3 * i : 3 * i + 1] + block[:, 3 * i + 1 : 3 * i + 2] + block[:, 3 * i + 2 : 3 * i + 3]
        for i in range(3)
    ]


def owner_of(row, order):
    mask, place = jnp.zeros_like(row), 0
    for low, count in order:
        mask = mask | (((row >> place) & ((1 << count) - 1)) << low)
        place += count
    return mask


def load_kernel(count, *refs):
    ins, outs, sems = refs[:count], refs[count : 2 * count], refs[2 * count]
    copies = [
        pltpu.make_async_copy(src, dst, sems.at[i]) for i, (src, dst) in enumerate(zip(ins, outs))
    ]
    for copy in copies:
        copy.start()
    for copy in copies:
        copy.wait()


def stack_kernel(*refs):
    *ins, out = refs
    out[...] = jnp.concatenate([ref[...] for ref in ins], 0)


def give_kernel(order, tok_dev, *refs):
    *hidden_refs, weight_ref, targets_ref, give_ref, probs_ref, stats_ref = refs
    hidden = jnp.concatenate([ref[...] for ref in hidden_refs], 0)
    rows, depth = hidden.shape
    vocab = weight_ref.shape[0]
    half = rows // 2
    me = lax.axis_index(AXES)
    logits = lax.dot_general(
        hidden, weight_ref[...], (((1,), (1,)), ((), ())), preferred_element_type=F32
    )
    tokens = targets_ref.shape[1]
    row = lax.broadcasted_iota(jnp.int32, (rows, tokens), 0)
    token = (me ^ owner_of(row // tok_dev, order)) * tok_dev + row % tok_dev
    column = lax.broadcasted_iota(jnp.int32, (rows, tokens), 1)
    target = jnp.sum(
        jnp.where(column == token, targets_ref[...], 0), axis=1, keepdims=True
    ) - me * vocab
    hit = lax.broadcasted_iota(jnp.int32, (rows, vocab), 1) == target
    largest = jnp.max(logits, axis=1, keepdims=True)
    shifted = jnp.exp(logits - largest)
    total = jnp.sum(shifted, axis=1, keepdims=True)
    at_target = jnp.sum(jnp.where(hit, logits, 0.0), axis=1, keepdims=True)
    shifted = shifted.astype(BF16)
    hot = hit.astype(F32).astype(BF16)
    stats = pack((largest, total, at_target), rows)
    probs_ref[:half] = shifted[:half]
    probs_ref[half:] = hot[:half]
    stats_ref[...] = stats[:half]
    give_ref[:, 2 * depth :] = stats[half:]
    both = jnp.concatenate([shifted[half:], hot[half:]], 0)
    step = min(depth, 1024)
    for at in range(0, depth, step):
        out = jnp.dot(both, weight_ref[:, at : at + step], preferred_element_type=F32).astype(BF16)
        give_ref[:, at : at + step] = out[:half]
        give_ref[:, depth + at : depth + at + step] = out[half:]


def keep_kernel(probs_ref, weight_ref, summed_ref, hot_ref):
    half, depth = summed_ref.shape
    step = min(depth, 1024)
    for at in range(0, depth, step):
        out = jnp.dot(probs_ref[...], weight_ref[:, at : at + step], preferred_element_type=F32)
        summed_ref[:, at : at + step] = out[:half]
        hot_ref[:, at : at + step] = out[half:].astype(BF16)


def views(ref):
    depth = (ref.shape[1] - LANES) // 2
    return ref.at[:, :depth], ref.at[:, depth : 2 * depth], ref.at[:, 2 * depth :]


def merged(stats_refs):
    stats = [unpack(ref[...]) for ref in stats_refs]
    largest = functools.reduce(jnp.maximum, [s[0] for s in stats])
    scales = [jnp.exp(s[0] - largest) for s in stats]
    total = sum(a * s[1] for a, s in zip(scales, stats))
    at_target = sum(s[2] for s in stats)
    return scales, largest, total, at_target


def merge(sources, outs):
    scales, *stats = merged([source[2] for source in sources])
    rows, depth = sources[0][0].shape
    each = rows // len(outs)

    def put(at, size, value):
        for i, out in enumerate(outs):
            out[:, at : at + size] = value[i * each : (i + 1) * each]

    put(2 * depth, LANES, pack(stats, rows))
    put(0, depth, sum(a * s[0][...].astype(F32) for a, s in zip(scales, sources)).astype(BF16))
    put(depth, depth, sum(s[1][...].astype(F32) for s in sources).astype(BF16))


def first_merge_kernel(summed, hot, stats, taken, *outs):
    merge([(summed, hot, stats), views(taken)], outs)


def merge_kernel(parts, *refs):
    merge([views(ref) for ref in refs[:parts]], refs[parts:])


def last_kernel(parts, *refs):
    sources, (scale_ref, loss_ref, grad_ref) = [views(ref) for ref in refs[:parts]], refs[parts:]
    scales, largest, total, at_target = merged([source[2] for source in sources])
    loss_ref[...] = jnp.broadcast_to(largest + jnp.log(total) - at_target, loss_ref.shape)
    summed = sum(a * s[0][...].astype(F32) for a, s in zip(scales, sources))
    hot = sum(s[1][...].astype(F32) for s in sources)
    sums = summed / total - hot
    for i in range(grad_ref.shape[0]):
        grad_ref[i : i + 1] = (scale_ref[i] * sums[i : i + 1]).astype(BF16)


def call(kernel, ins, outs, flops=0, specs=None, scratch=(), params=PARAMS):
    return pl.pallas_call(
        kernel,
        out_shape=outs,
        in_specs=specs or [VMEM] * len(ins),
        out_specs=jax.tree.map(lambda _: VMEM, outs),
        scratch_shapes=list(scratch),
        compiler_params=params,
        cost_estimate=pl.CostEstimate(flops=flops, bytes_accessed=flops // 64, transcendentals=0),
    )(*ins)


def shards(devices, hidden, weight, targets, loss_grad):
    return staged(devices, hidden, weight, targets[None, :], loss_grad)


def exchange(pieces, group, devices):
    got = {}
    for k in reversed(range(1, 1 << group[1])):
        got[k] = swap(pieces[k], k << group[0], devices)
    return [got[k] for k in range(1, 1 << group[1])]


def load(arrays, params):
    return call(
        functools.partial(load_kernel, len(arrays)),
        arrays,
        tuple(jax.ShapeDtypeStruct(a.shape, a.dtype) for a in arrays),
        flops=64 * sum(a.size for a in arrays),
        specs=[HBM] * len(arrays),
        params=params,
        scratch=[pltpu.SemaphoreType.DMA((len(arrays),))],
    )


def staged(devices, hidden, weight, targets, loss_grad):
    tok_dev, depth = hidden.shape
    vocab = weight.shape[0]
    groups = bit_groups(devices)
    mine, targets = load((hidden, targets), PARAMS)
    (weight,) = load((weight,), LOAD_PARAMS)
    whole, own = hidden, mine
    for i, group in enumerate(groups):
        got = exchange([whole] * (1 << group[1]), group, devices)
        if i + 1 == len(groups):
            break
        size = (1 + len(got)) * whole.shape[0]
        whole = own = call(stack_kernel, [own, *got], jax.ShapeDtypeStruct((size, depth), BF16))
    rows = devices * tok_dev
    half, width = rows // 2, 2 * depth + LANES
    flops = 4 * half * vocab * depth
    give, probs, stats = call(
        functools.partial(give_kernel, groups, tok_dev),
        [own, *got, weight, targets],
        (
            jax.ShapeDtypeStruct((half, width), BF16),
            jax.ShapeDtypeStruct((rows, vocab), BF16),
            jax.ShapeDtypeStruct((half, LANES), BF16),
        ),
        flops=3 * flops,
    )
    (taken,) = exchange([None, give], groups[-1], devices)
    summed, hot = call(
        keep_kernel,
        [probs, weight],
        (jax.ShapeDtypeStruct((half, depth), F32), jax.ShapeDtypeStruct((half, depth), BF16)),
        flops=flops,
    )
    kernel, parts = first_merge_kernel, [summed, hot, stats, taken]
    for group in reversed(groups[:-1]):
        peers = 1 << group[1]
        size = parts[0].shape[0] // peers
        outs = call(kernel, parts, (jax.ShapeDtypeStruct((size, width), BF16),) * peers)
        parts = [outs[0]] + exchange(outs, group, devices)
        kernel = functools.partial(merge_kernel, len(parts))
    loss, grad = call(
        functools.partial(last_kernel, len(parts)),
        [*parts, loss_grad],
        (
            jax.ShapeDtypeStruct((tok_dev, LANES), F32),
            jax.ShapeDtypeStruct((tok_dev, depth), BF16),
        ),
        specs=[VMEM] * len(parts) + [SMEM],
    )
    return loss[:, 0], grad


def solution(mesh):
    devices = math.prod(mesh.shape[axis] for axis in AXES)
    return jax.shard_map(
        functools.partial(shards, devices),
        mesh=mesh,
        in_specs=(P(AXES, None), P(AXES, None), P(), P(AXES)),
        out_specs=(P(AXES), P(AXES, None)),
        check_vma=False,
    )
```

```python
import functools
import math

import jax
import jax.numpy as jnp
from jax import lax
from jax.experimental import pallas as pl
from jax.experimental.pallas import tpu as pltpu
from jax.sharding import PartitionSpec as P


AXES = ("section", "tensor")
LANES = 128
F32 = jnp.float32
BF16 = jnp.bfloat16
VMEM = pl.BlockSpec(memory_space=pltpu.VMEM)
HBM = pl.BlockSpec(memory_space=pl.ANY)
SMEM = pl.BlockSpec(memory_space=pltpu.SMEM)
PARAMS = pltpu.CompilerParams(vmem_limit_bytes=32 * 2**20)
LOAD_PARAMS = pltpu.CompilerParams(vmem_limit_bytes=44 * 2**20)


def bit_groups(devices):
    bits = devices.bit_length() - 1
    groups, top = [], bits
    while top > 1:
        low = max(1, top - 2)
        groups.append((low, top - low))
        top = low
    return groups + [(0, 1)]


def swap(array, mask, devices):
    return lax.ppermute(array, AXES, [(i, i ^ mask) for i in range(devices)])


def split3(value):
    parts = []
    for _ in range(3):
        part = value.astype(BF16).astype(F32)
        parts.append(part)
        value = value - part
    return parts


def pack(values, rows):
    lane = lax.broadcasted_iota(jnp.int32, (rows, LANES), 1)
    block = jnp.zeros((rows, LANES), F32)
    for i, part in enumerate(p for v in values for p in split3(v)):
        block = jnp.where(lane == i, part, block)
    return block.astype(BF16)


def unpack(block):
    block = block.astype(F32)
    return [
        block[:, 3 * i : 3 * i + 1] + block[:, 3 * i + 1 : 3 * i + 2] + block[:, 3 * i + 2 : 3 * i + 3]
        for i in range(3)
    ]


def owner_of(row, order):
    mask, place = jnp.zeros_like(row), 0
    for low, count in order:
        part = (row >> place) & ((1 << count) - 1)
        mask = mask ^ (part << low)
        if low:
            mask = mask ^ (part > 0).astype(jnp.int32)
        place += count
    return mask


def load_kernel(count, *refs):
    ins, outs, sems = refs[:count], refs[count : 2 * count], refs[2 * count]
    copies = [
        pltpu.make_async_copy(src, dst, sems.at[i]) for i, (src, dst) in enumerate(zip(ins, outs))
    ]
    for copy in copies:
        copy.start()
    for copy in copies:
        copy.wait()


def stack_kernel(*refs):
    *ins, out = refs
    out[...] = jnp.concatenate([ref[...] for ref in ins], 0)


def give_kernel(order, tok_dev, *refs):
    *hidden_refs, weight_ref, targets_ref, give_ref, probs_ref, stats_ref = refs
    hidden = jnp.concatenate([ref[...] for ref in hidden_refs], 0)
    rows, depth = hidden.shape
    vocab = weight_ref.shape[0]
    half = rows // 2
    me = lax.axis_index(AXES)
    logits = lax.dot_general(
        hidden, weight_ref[...], (((1,), (1,)), ((), ())), preferred_element_type=F32
    )
    tokens = targets_ref.shape[1]
    row = lax.broadcasted_iota(jnp.int32, (rows, tokens), 0)
    token = (me ^ owner_of(row // tok_dev, order)) * tok_dev + row % tok_dev
    column = lax.broadcasted_iota(jnp.int32, (rows, tokens), 1)
    target = jnp.sum(
        jnp.where(column == token, targets_ref[...], 0), axis=1, keepdims=True
    ) - me * vocab
    hit = lax.broadcasted_iota(jnp.int32, (rows, vocab), 1) == target
    largest = jnp.max(logits, axis=1, keepdims=True)
    shifted = jnp.exp(logits - largest)
    total = jnp.sum(shifted, axis=1, keepdims=True)
    at_target = jnp.sum(jnp.where(hit, logits, 0.0), axis=1, keepdims=True)
    shifted = shifted.astype(BF16)
    hot = hit.astype(F32).astype(BF16)
    stats = pack((largest, total, at_target), rows)
    probs_ref[:half] = shifted[:half]
    probs_ref[half:] = hot[:half]
    stats_ref[...] = stats[:half]
    give_ref[:, 2 * depth :] = stats[half:]
    both = jnp.concatenate([shifted[half:], hot[half:]], 0)
    step = min(depth, 1024)
    for at in range(0, depth, step):
        out = jnp.dot(both, weight_ref[:, at : at + step], preferred_element_type=F32).astype(BF16)
        give_ref[:, at : at + step] = out[:half]
        give_ref[:, depth + at : depth + at + step] = out[half:]


def keep_kernel(probs_ref, weight_ref, summed_ref, hot_ref):
    half, depth = summed_ref.shape
    step = min(depth, 1024)
    for at in range(0, depth, step):
        out = jnp.dot(probs_ref[...], weight_ref[:, at : at + step], preferred_element_type=F32)
        summed_ref[:, at : at + step] = out[:half]
        hot_ref[:, at : at + step] = out[half:].astype(BF16)


def views(ref):
    depth = (ref.shape[1] - LANES) // 2
    return ref.at[:, :depth], ref.at[:, depth : 2 * depth], ref.at[:, 2 * depth :]


def merged(stats_refs):
    stats = [unpack(ref[...]) for ref in stats_refs]
    largest = functools.reduce(jnp.maximum, [s[0] for s in stats])
    scales = [jnp.exp(s[0] - largest) for s in stats]
    total = sum(a * s[1] for a, s in zip(scales, stats))
    at_target = sum(s[2] for s in stats)
    return scales, largest, total, at_target


def merge(sources, outs):
    scales, *stats = merged([source[2] for source in sources])
    rows, depth = sources[0][0].shape
    each = rows // len(outs)

    def put(at, size, value):
        for i, out in enumerate(outs):
            out[:, at : at + size] = value[i * each : (i + 1) * each]

    put(2 * depth, LANES, pack(stats, rows))
    put(0, depth, sum(a * s[0][...].astype(F32) for a, s in zip(scales, sources)).astype(BF16))
    put(depth, depth, sum(s[1][...].astype(F32) for s in sources).astype(BF16))


def first_merge_kernel(summed, hot, stats, taken, *outs):
    merge([(summed, hot, stats), views(taken)], outs)


def merge_kernel(parts, *refs):
    merge([views(ref) for ref in refs[:parts]], refs[parts:])


def last_kernel(parts, *refs):
    sources, (scale_ref, loss_ref, grad_ref) = [views(ref) for ref in refs[:parts]], refs[parts:]
    scales, largest, total, at_target = merged([source[2] for source in sources])
    loss_ref[...] = jnp.broadcast_to(largest + jnp.log(total) - at_target, loss_ref.shape)
    summed = sum(a * s[0][...].astype(F32) for a, s in zip(scales, sources))
    hot = sum(s[1][...].astype(F32) for s in sources)
    sums = summed / total - hot
    for i in range(grad_ref.shape[0]):
        grad_ref[i : i + 1] = (scale_ref[i] * sums[i : i + 1]).astype(BF16)


def call(kernel, ins, outs, flops=0, specs=None, scratch=(), params=PARAMS):
    return pl.pallas_call(
        kernel,
        out_shape=outs,
        in_specs=specs or [VMEM] * len(ins),
        out_specs=jax.tree.map(lambda _: VMEM, outs),
        scratch_shapes=list(scratch),
        compiler_params=params,
        cost_estimate=pl.CostEstimate(flops=flops, bytes_accessed=flops // 64, transcendentals=0),
    )(*ins)


def shards(devices, hidden, weight, targets, loss_grad):
    return staged(devices, hidden, weight, targets[None, :], loss_grad)


def exchange(pieces, group, devices):
    got = {}
    for k in reversed(range(1, 1 << group[1])):
        got[k] = swap(pieces[k], k << group[0] | 1, devices)
    return [got[k] for k in range(1, 1 << group[1])]


def load(arrays, params):
    return call(
        functools.partial(load_kernel, len(arrays)),
        arrays,
        tuple(jax.ShapeDtypeStruct(a.shape, a.dtype) for a in arrays),
        flops=64 * sum(a.size for a in arrays),
        specs=[HBM] * len(arrays),
        params=params,
        scratch=[pltpu.SemaphoreType.DMA((len(arrays),))],
    )


def staged(devices, hidden, weight, targets, loss_grad):
    tok_dev, depth = hidden.shape
    vocab = weight.shape[0]
    groups = bit_groups(devices)
    mine, targets = load((hidden, targets), PARAMS)
    (weight,) = load((weight,), LOAD_PARAMS)
    whole, own = hidden, mine
    for i, group in enumerate(groups):
        got = exchange([whole] * (1 << group[1]), group, devices)
        if i + 1 == len(groups):
            break
        size = (1 + len(got)) * whole.shape[0]
        whole = own = call(stack_kernel, [own, *got], jax.ShapeDtypeStruct((size, depth), BF16))
    rows = devices * tok_dev
    half, width = rows // 2, 2 * depth + LANES
    flops = 4 * half * vocab * depth
    give, probs, stats = call(
        functools.partial(give_kernel, groups, tok_dev),
        [own, *got, weight, targets],
        (
            jax.ShapeDtypeStruct((half, width), BF16),
            jax.ShapeDtypeStruct((rows, vocab), BF16),
            jax.ShapeDtypeStruct((half, LANES), BF16),
        ),
        flops=3 * flops,
    )
    (taken,) = exchange([None, give], groups[-1], devices)
    summed, hot = call(
        keep_kernel,
        [probs, weight],
        (jax.ShapeDtypeStruct((half, depth), F32), jax.ShapeDtypeStruct((half, depth), BF16)),
        flops=flops,
    )
    kernel, parts = first_merge_kernel, [summed, hot, stats, taken]
    for group in reversed(groups[:-1]):
        peers = 1 << group[1]
        size = parts[0].shape[0] // peers
        outs = call(kernel, parts, (jax.ShapeDtypeStruct((size, width), BF16),) * peers)
        parts = [outs[0]] + exchange(outs, group, devices)
        kernel = functools.partial(merge_kernel, len(parts))
    loss, grad = call(
        functools.partial(last_kernel, len(parts)),
        [*parts, loss_grad],
        (
            jax.ShapeDtypeStruct((tok_dev, LANES), F32),
            jax.ShapeDtypeStruct((tok_dev, depth), BF16),
        ),
        specs=[VMEM] * len(parts) + [SMEM],
    )
    return loss[:, 0], grad


def solution(mesh):
    devices = math.prod(mesh.shape[axis] for axis in AXES)
    return jax.shard_map(
        functools.partial(shards, devices),
        mesh=mesh,
        in_specs=(P(AXES, None), P(AXES, None), P(), P(AXES)),
        out_specs=(P(AXES), P(AXES, None)),
        check_vma=False,
    )
```

```python
import functools
import math

import jax
import jax.numpy as jnp
from jax import lax
from jax.experimental import pallas as pl
from jax.experimental.pallas import tpu as pltpu
from jax.sharding import PartitionSpec as P


AXES = ("section", "tensor")
LANES = 128
PIECES = 4
F32 = jnp.float32
BF16 = jnp.bfloat16
VMEM = pl.BlockSpec(memory_space=pltpu.VMEM)
HBM = pl.BlockSpec(memory_space=pl.ANY)
SMEM = pl.BlockSpec(memory_space=pltpu.SMEM)
PARAMS = pltpu.CompilerParams(vmem_limit_bytes=32 * 2**20)
LOAD_PARAMS = pltpu.CompilerParams(vmem_limit_bytes=44 * 2**20)


def bit_groups(devices):
    bits = devices.bit_length() - 1
    groups, top = [], bits
    while top > 1:
        low = max(1, top - 2)
        groups.append((low, top - low))
        top = low
    return groups + [(0, 1)]


def swap(array, mask, devices):
    return lax.ppermute(array, AXES, [(i, i ^ mask) for i in range(devices)])


def split3(value):
    parts = []
    for _ in range(3):
        part = value.astype(BF16).astype(F32)
        parts.append(part)
        value = value - part
    return parts


def pack(values, rows):
    lane = lax.broadcasted_iota(jnp.int32, (rows, LANES), 1)
    block = jnp.zeros((rows, LANES), F32)
    for i, part in enumerate(p for v in values for p in split3(v)):
        block = jnp.where(lane == i, part, block)
    return block.astype(BF16)


def unpack(block):
    block = block.astype(F32)
    return [
        block[:, 3 * i : 3 * i + 1] + block[:, 3 * i + 1 : 3 * i + 2] + block[:, 3 * i + 2 : 3 * i + 3]
        for i in range(3)
    ]


def owner_of(row, order):
    mask, place = jnp.zeros_like(row), 0
    for low, count in order:
        part = (row >> place) & ((1 << count) - 1)
        mask = mask ^ (part << low)
        if low:
            mask = mask ^ (part > 0).astype(jnp.int32)
        place += count
    return mask


def load_kernel(count, *refs):
    ins, outs, sems = refs[:count], refs[count : 2 * count], refs[2 * count]
    copies = []
    for i, (src, dst) in enumerate(zip(ins, outs)):
        rows = src.shape[0]
        cuts = PIECES if rows % (8 * PIECES) == 0 else 1
        for k in range(cuts):
            part = pl.ds(k * (rows // cuts), rows // cuts)
            copies.append(pltpu.make_async_copy(src.at[part], dst.at[part], sems.at[i * PIECES + k]))
    for copy in copies:
        copy.start()
    for copy in copies:
        copy.wait()


def stack_kernel(*refs):
    *ins, out = refs
    out[...] = jnp.concatenate([ref[...] for ref in ins], 0)


def give_kernel(order, tok_dev, *refs):
    *hidden_refs, weight_ref, targets_ref, give_ref, probs_ref, stats_ref = refs
    hidden = jnp.concatenate([ref[...] for ref in hidden_refs], 0)
    rows, depth = hidden.shape
    vocab = weight_ref.shape[0]
    half = rows // 2
    me = lax.axis_index(AXES)
    logits = lax.dot_general(
        hidden, weight_ref[...], (((1,), (1,)), ((), ())), preferred_element_type=F32
    )
    tokens = targets_ref.shape[1]
    row = lax.broadcasted_iota(jnp.int32, (rows, tokens), 0)
    token = (me ^ owner_of(row // tok_dev, order)) * tok_dev + row % tok_dev
    column = lax.broadcasted_iota(jnp.int32, (rows, tokens), 1)
    target = jnp.sum(
        jnp.where(column == token, targets_ref[...], 0), axis=1, keepdims=True
    ) - me * vocab
    hit = lax.broadcasted_iota(jnp.int32, (rows, vocab), 1) == target
    largest = jnp.max(logits, axis=1, keepdims=True)
    shifted = jnp.exp(logits - largest)
    total = jnp.sum(shifted, axis=1, keepdims=True)
    at_target = jnp.sum(jnp.where(hit, logits, 0.0), axis=1, keepdims=True)
    shifted = shifted.astype(BF16)
    hot = hit.astype(F32).astype(BF16)
    stats = pack((largest, total, at_target), rows)
    probs_ref[:half] = shifted[:half]
    probs_ref[half:] = hot[:half]
    stats_ref[...] = stats[:half]
    give_ref[:, 2 * depth :] = stats[half:]
    both = jnp.concatenate([shifted[half:], hot[half:]], 0)
    step = min(depth, 1024)
    for at in range(0, depth, step):
        out = jnp.dot(both, weight_ref[:, at : at + step], preferred_element_type=F32).astype(BF16)
        give_ref[:, at : at + step] = out[:half]
        give_ref[:, depth + at : depth + at + step] = out[half:]


def keep_kernel(probs_ref, weight_ref, summed_ref, hot_ref):
    half, depth = summed_ref.shape
    step = min(depth, 1024)
    for at in range(0, depth, step):
        out = jnp.dot(probs_ref[...], weight_ref[:, at : at + step], preferred_element_type=F32)
        summed_ref[:, at : at + step] = out[:half]
        hot_ref[:, at : at + step] = out[half:].astype(BF16)


def views(ref):
    depth = (ref.shape[1] - LANES) // 2
    return ref.at[:, :depth], ref.at[:, depth : 2 * depth], ref.at[:, 2 * depth :]


def merged(stats_refs):
    stats = [unpack(ref[...]) for ref in stats_refs]
    largest = functools.reduce(jnp.maximum, [s[0] for s in stats])
    scales = [jnp.exp(s[0] - largest) for s in stats]
    total = sum(a * s[1] for a, s in zip(scales, stats))
    at_target = sum(s[2] for s in stats)
    return scales, largest, total, at_target


def merge(sources, outs):
    scales, *stats = merged([source[2] for source in sources])
    rows, depth = sources[0][0].shape
    each = rows // len(outs)

    def put(at, size, value):
        for i, out in enumerate(outs):
            out[:, at : at + size] = value[i * each : (i + 1) * each]

    put(2 * depth, LANES, pack(stats, rows))
    put(0, depth, sum(a * s[0][...].astype(F32) for a, s in zip(scales, sources)).astype(BF16))
    put(depth, depth, sum(s[1][...].astype(F32) for s in sources).astype(BF16))


def first_merge_kernel(summed, hot, stats, taken, *outs):
    merge([(summed, hot, stats), views(taken)], outs)


def merge_kernel(parts, *refs):
    merge([views(ref) for ref in refs[:parts]], refs[parts:])


def last_kernel(parts, *refs):
    sources, (scale_ref, loss_ref, grad_ref) = [views(ref) for ref in refs[:parts]], refs[parts:]
    scales, largest, total, at_target = merged([source[2] for source in sources])
    loss_ref[...] = jnp.broadcast_to(largest + jnp.log(total) - at_target, loss_ref.shape)
    summed = sum(a * s[0][...].astype(F32) for a, s in zip(scales, sources))
    hot = sum(s[1][...].astype(F32) for s in sources)
    sums = summed / total - hot
    for i in range(grad_ref.shape[0]):
        grad_ref[i : i + 1] = (scale_ref[i] * sums[i : i + 1]).astype(BF16)


def call(kernel, ins, outs, flops=0, specs=None, scratch=(), params=PARAMS):
    return pl.pallas_call(
        kernel,
        out_shape=outs,
        in_specs=specs or [VMEM] * len(ins),
        out_specs=jax.tree.map(lambda _: VMEM, outs),
        scratch_shapes=list(scratch),
        compiler_params=params,
        cost_estimate=pl.CostEstimate(flops=flops, bytes_accessed=flops // 64, transcendentals=0),
    )(*ins)


def shards(devices, hidden, weight, targets, loss_grad):
    return staged(devices, hidden, weight, targets[None, :], loss_grad)


def exchange(pieces, group, devices):
    got = {}
    for k in reversed(range(1, 1 << group[1])):
        got[k] = swap(pieces[k], k << group[0] | 1, devices)
    return [got[k] for k in range(1, 1 << group[1])]


def load(arrays, params):
    return call(
        functools.partial(load_kernel, len(arrays)),
        arrays,
        tuple(jax.ShapeDtypeStruct(a.shape, a.dtype) for a in arrays),
        flops=64 * sum(a.size for a in arrays),
        specs=[HBM] * len(arrays),
        params=params,
        scratch=[pltpu.SemaphoreType.DMA((len(arrays) * PIECES,))],
    )


def staged(devices, hidden, weight, targets, loss_grad):
    tok_dev, depth = hidden.shape
    vocab = weight.shape[0]
    groups = bit_groups(devices)
    mine, targets = load((hidden, targets), PARAMS)
    (weight,) = load((weight,), LOAD_PARAMS)
    whole, own = hidden, mine
    for i, group in enumerate(groups):
        got = exchange([whole] * (1 << group[1]), group, devices)
        if i + 1 == len(groups):
            break
        size = (1 + len(got)) * whole.shape[0]
        whole = own = call(stack_kernel, [own, *got], jax.ShapeDtypeStruct((size, depth), BF16))
    rows = devices * tok_dev
    half, width = rows // 2, 2 * depth + LANES
    flops = 4 * half * vocab * depth
    give, probs, stats = call(
        functools.partial(give_kernel, groups, tok_dev),
        [own, *got, weight, targets],
        (
            jax.ShapeDtypeStruct((half, width), BF16),
            jax.ShapeDtypeStruct((rows, vocab), BF16),
            jax.ShapeDtypeStruct((half, LANES), BF16),
        ),
        flops=3 * flops,
    )
    (taken,) = exchange([None, give], groups[-1], devices)
    summed, hot = call(
        keep_kernel,
        [probs, weight],
        (jax.ShapeDtypeStruct((half, depth), F32), jax.ShapeDtypeStruct((half, depth), BF16)),
        flops=flops,
    )
    kernel, parts = first_merge_kernel, [summed, hot, stats, taken]
    for group in reversed(groups[:-1]):
        peers = 1 << group[1]
        size = parts[0].shape[0] // peers
        outs = call(kernel, parts, (jax.ShapeDtypeStruct((size, width), BF16),) * peers)
        parts = [outs[0]] + exchange(outs, group, devices)
        kernel = functools.partial(merge_kernel, len(parts))
    loss, grad = call(
        functools.partial(last_kernel, len(parts)),
        [*parts, loss_grad],
        (
            jax.ShapeDtypeStruct((tok_dev, LANES), F32),
            jax.ShapeDtypeStruct((tok_dev, depth), BF16),
        ),
        specs=[VMEM] * len(parts) + [SMEM],
    )
    return loss[:, 0], grad


def solution(mesh):
    devices = math.prod(mesh.shape[axis] for axis in AXES)
    return jax.shard_map(
        functools.partial(shards, devices),
        mesh=mesh,
        in_specs=(P(AXES, None), P(AXES, None), P(), P(AXES)),
        out_specs=(P(AXES), P(AXES, None)),
        check_vma=False,
    )
```
